32 devices in a mesh: fluid: 4 (over y, x), solid: 8 (over z, core).
Axes of the slice: x: 2, y: 2, z: 4, core: 2. Of those that a mesh axis runs over, the one named last changes fastest.
Arguments:
- fluid_flux: bfloat16 [3, 2048, 128], P(None, ('fluid', 'solid')), may hold values from -6 to 6
- margin_blocks: bfloat16 [5120, 128, 128], P(('fluid', 'solid')), may hold values from 0 to 0.046875
- block_fluid: int32 [5120], P(('fluid', 'solid')), may hold values from 0 to 63
- block_solid: int32 [5120], P(('fluid', 'solid')), may hold values from 0 to 255, as said below
- diag_blocks: float32 [256, 128, 128], P('solid'), may hold values from -3 to 18, as said below
- couple_blocks: float32 [256, 128, 128], P('solid'), may hold values from -0.15 to 0.15
- couple_offset: int32 [256], P('solid'), may hold values from 1 to 16
Outputs:
- mapped: float32 [3, 256, 128], P(None, 'solid')
- nodal: float32 [3, 256, 128], P(None, 'solid')
The draws below stay inside these ranges and needn't reach their ends.
Inputs may be any that keep to these rules, and one draw needn't show every extreme that they name: `block_solid`: the solid tiles of solid index s are s * 32 to (s + 1) * 32 - 1. Among the 160 blocks of one device at most 50 have solid tiles of one solid index, and exactly 50 do for some index. block_fluid indexes the 64 fluid tiles of the device that holds the block. `diag_blocks`: each diagonal block is symmetric.
All inputs are finite; a program needn't handle non-finite values.
Results may differ from the reference program's by a relative error of at most 0.0003.
Values sent between devices are 32-bit elements; how exact they have to be, the bound alone decides.
A program may use at most 64 MiB of HBM per device.

```python
import math
import jax
import jax.numpy as jnp
from jax import lax

TILE = 128
F = 3
FT_DEV = 64
B_DEV = 160
ST_DEV = 32
HALO = 16
ITERS = 3
FT = 2048
BLOCKS = 5120
ST = 256
CAP = 50
N_FLUID = 4
N_SOLID = 8


def draw_block_solid(key, part):
    devices = N_FLUID * N_SOLID
    slots = N_SOLID * CAP

    def one_device(index):
        device_key = jax.random.fold_in(jax.random.fold_in(key, 101), index)
        key_forced, key_noise, key_order, key_tile = jax.random.split(device_key, 4)
        slot_owner = jnp.arange(slots, dtype=jnp.int32) // CAP
        home_owner = index % N_SOLID
        forced = jax.random.randint(key_forced, (), 0, N_SOLID)
        distance = jnp.abs(slot_owner - home_owner)
        distance = jnp.minimum(distance, N_SOLID - distance)
        preference = jnp.where(slot_owner == forced, 2, jnp.where(distance <= 1, 1, 0))
        noise_bits = jax.random.randint(key_noise, (slots,), 0, 2 ** 18)
        scores = (preference * 2 ** 18 + noise_bits) * slots + jnp.arange(slots, dtype=jnp.int32)
        chosen_slots = lax.top_k(scores, B_DEV)[1]
        chosen_slots = jax.random.permutation(key_order, chosen_slots)
        tile_pick = jax.random.randint(key_tile, (B_DEV,), 0, ST_DEV)
        return chosen_slots // CAP * ST_DEV + tile_pick
    return jax.vmap(one_device)(jnp.arange(devices, dtype=jnp.int32)).reshape(-1).astype(jnp.int32)


def draw_diag_blocks(key, part):
    total_tiles = ST_DEV * N_SOLID
    key_rough, key_diagonal = jax.random.split(jax.random.fold_in(key, 7))
    spread_scale = 3.0 / math.sqrt(TILE)
    base_draw = jax.random.uniform(key_diagonal, (total_tiles, TILE), jnp.float32, 0.0, 1.0)
    rough_part = jax.random.uniform(key_rough, (total_tiles, TILE, TILE), jnp.float32, -spread_scale, spread_scale)
    diagonal = 8.0 + 10.0 * base_draw ** 4
    upper_part = jnp.triu(rough_part, 1)
    symmetric = upper_part + jnp.swapaxes(upper_part, 1, 2)
    return symmetric + diagonal[:, :, None] * jnp.eye(TILE, dtype=jnp.float32)[None, :, :]


def draw_couple_blocks(key, part):
    total_tiles = ST_DEV * N_SOLID
    key_size = jax.random.fold_in(jax.random.fold_in(key, 13), 0)
    return jax.random.uniform(key_size, (total_tiles, TILE, TILE), jnp.float32, -0.15, 0.15)


def set_ends(result, own_key, smallest, top_value):
    spot = [jax.random.randint(jax.random.fold_in(own_key, axis), (), 0, length) for axis, length in enumerate(result.shape)]
    longest = result.shape.index(max(result.shape))
    neighbour = spot[:longest] + [(spot[longest] + 1) % result.shape[longest]] + spot[longest + 1:]
    return result.at[tuple(spot)].set(smallest).at[tuple(neighbour)].set(top_value)


def levels(rng, extent, cuts, smallest, high):
    level, own = 1.0, jax.random.fold_in(rng, 6)
    for position, blocks in cuts:
        heights = jnp.exp(jax.random.uniform(jax.random.fold_in(own, position), (blocks,), jnp.float32, smallest / len(cuts), high / len(cuts)))
        level = level * jnp.repeat(heights, extent[position] // blocks).reshape([-1 if axis == position else 1 for axis in range(len(extent))])
    return level


def scatter_about(key, extent, scale, bound, cuts=(), held_as=jnp.bfloat16):
    level = levels(key, extent, cuts, -0.22, 0.18) if cuts else 1.0
    values = jax.random.normal(key, extent, jnp.float32) * scale * level
    return jnp.minimum(jnp.maximum(values, -bound), bound).astype(held_as)


def setup_inputs(seed: int = 0) -> dict:
    seeds = jax.random.split(jax.random.key(seed), 8)
    return {
        "fluid_flux": scatter_about(seeds[0], (F, FT, TILE), 1.0, 6.0, ((1, 32),)),
        "margin_blocks": jnp.clip(0.046875 * jax.random.uniform(seeds[1], (BLOCKS, TILE, TILE), jnp.float32) ** levels(seeds[1], (BLOCKS, TILE, TILE), ((0, 32),), -0.2, 0.2), 0.0, 0.046875).astype(jnp.bfloat16),
        "block_fluid": set_ends(jax.random.randint(seeds[2], (BLOCKS,), 0, FT_DEV), jax.random.fold_in(seeds[2], 1), 0, FT_DEV - 1).astype(jnp.int32),
        "block_solid": draw_block_solid(jax.random.fold_in(seeds[7], 71), 0),
        "diag_blocks": draw_diag_blocks(jax.random.fold_in(seeds[7], 71), 0),
        "couple_blocks": draw_couple_blocks(jax.random.fold_in(seeds[7], 71), 0),
        "couple_offset": set_ends(jax.random.randint(seeds[6], (ST,), 1, HALO + 1), jax.random.fold_in(seeds[6], 1), 1, HALO).astype(jnp.int32),
    }


highest = lax.Precision.HIGHEST


def apply_mass(vector, diag_blocks, couple_blocks, couple_offset):
    fields = vector.shape[0]
    total_tiles = vector.shape[1]
    own_part = jnp.einsum('tij,ftj->fti', diag_blocks, vector, precision=highest)
    padded = jnp.concatenate([vector, jnp.zeros((fields, HALO, TILE), jnp.float32)], axis=1)
    picked = jnp.zeros_like(vector)
    for offset in range(1, HALO + 1):
        offset_hit = (couple_offset == offset)[None, :, None]
        picked = picked + jnp.where(offset_hit, padded[:, offset:offset + total_tiles], 0.0)
    ahead_part = jnp.einsum('tij,ftj->fti', couple_blocks, picked, precision=highest)
    back_terms = jnp.einsum('tji,ftj->fti', couple_blocks, vector, precision=highest)
    spread = jnp.zeros_like(padded)
    for offset in range(1, HALO + 1):
        offset_hit = (couple_offset == offset)[None, :, None]
        moved = jnp.where(offset_hit, back_terms, 0.0)
        spread = spread + jnp.pad(moved, ((0, 0), (offset, HALO - offset), (0, 0)))
    return own_part + ahead_part + spread[:, :total_tiles]


def field_dots(first, second):
    return jnp.sum(first * second, axis=(1, 2))


def reference(fluid_flux, margin_blocks, block_fluid, block_solid, diag_blocks, couple_blocks, couple_offset):
    total_tiles = ST_DEV * N_SOLID
    devices = N_FLUID * N_SOLID
    fields = fluid_flux.shape[0]
    flux_dev = fluid_flux.reshape(fields, devices, FT_DEV, TILE).transpose(1, 0, 2, 3)
    blocks_dev = margin_blocks.reshape(devices, B_DEV, TILE, TILE)
    fluid_ids = block_fluid.reshape(devices, B_DEV)
    solid_ids = block_solid.reshape(devices, B_DEV)

    def accumulate(running, pieces):
        flux, blocks, fluid_rows, solid_rows = pieces
        chosen = jnp.take(flux, fluid_rows, axis=1).astype(jnp.float32)
        block_terms = jnp.einsum('fbi,bij->bfj', chosen, blocks.astype(jnp.float32), precision=highest)
        return running + jax.ops.segment_sum(block_terms, solid_rows, num_segments=total_tiles), None

    start = jnp.zeros((total_tiles, fields, TILE), jnp.float32)
    outcome = lax.scan(accumulate, start, (flux_dev, blocks_dev, fluid_ids, solid_ids))
    mapped = outcome[0].transpose(1, 0, 2)

    solution = jnp.zeros_like(mapped)
    residual = mapped
    direction = mapped
    norm_now = field_dots(residual, residual)
    for iteration in range(ITERS):
        image_field = apply_mass(direction, diag_blocks, couple_blocks, couple_offset)
        step_size = norm_now / field_dots(direction, image_field)
        solution = solution + step_size[:, None, None] * direction
        residual = residual - step_size[:, None, None] * image_field
        norm_next = field_dots(residual, residual)
        direction = residual + (norm_next / norm_now)[:, None, None] * direction
        norm_now = norm_next
    return mapped, solution
```

```python
import functools

import jax
import jax.numpy as jnp
from jax import lax
from jax.experimental import pallas as pl
from jax.experimental.pallas import tpu as pltpu
from jax.sharding import PartitionSpec as P

MESH = pl.DeviceIdType.MESH
ROWS = 8
LANES = 128


def gather_kernel(fluids, owners, chunks, group, fluid_ids, solid_ids, flux, blocks, out, faces, total):
    step = pl.program_id(0)
    fields = flux.shape[0]
    per_step = blocks.shape[0]
    own_tiles = chunks * fluids

    @pl.when(step == 0)
    def _():
        total[...] = jnp.zeros_like(total)
        faces[...] = jnp.zeros_like(faces)
        for field in range(fields):
            faces[pl.ds(field, flux.shape[1], stride=ROWS), :] = flux[field].astype(jnp.float32)

    def some(index, carry):
        terms = []
        for inner in range(group):
            here = index * group + inner
            start = pl.multiple_of(fluid_ids[step * per_step + here] * ROWS, ROWS)
            chosen = faces[pl.ds(start, ROWS), :].astype(jnp.bfloat16)
            terms.append(jnp.dot(chosen, blocks[here], preferred_element_type=jnp.float32))
        for inner in range(group):
            here = index * group + inner
            start = pl.multiple_of(solid_ids[step * per_step + here] * ROWS, ROWS)
            total[pl.ds(start, ROWS), :] += terms[inner]
        return carry

    lax.fori_loop(0, per_step // group, some, 0)

    @pl.when(step == pl.num_programs(0) - 1)
    def _():
        def one_owner(owner, carry):
            for part in range(fluids):
                for field in range(fields):
                    start = (owner * own_tiles + part * chunks) * ROWS + field
                    out[part, owner, field] = total[pl.ds(start, chunks, stride=ROWS), :]
            return carry

        lax.fori_loop(0, owners, one_owner, 0)


def gather_terms(flux, blocks, fluid_ids, solid_ids, fluids, owners, own_tiles):
    fields, fluid_tiles, width = flux.shape
    count = blocks.shape[0]
    steps = 4 if count % 32 == 0 else 1
    chunks = own_tiles // fluids
    return pl.pallas_call(
        functools.partial(gather_kernel, fluids, owners, chunks, 8),
        grid=(steps,),
        out_shape=jax.ShapeDtypeStruct((fluids, owners, fields, chunks, width), jnp.float32),
        in_specs=[
            pl.BlockSpec(memory_space=pltpu.SMEM),
            pl.BlockSpec(memory_space=pltpu.SMEM),
            pl.BlockSpec(memory_space=pltpu.VMEM),
            pl.BlockSpec((count // steps, width, width), lambda i: (i, 0, 0)),
        ],
        out_specs=pl.BlockSpec(memory_space=pltpu.VMEM),
        scratch_shapes=[
            pltpu.VMEM((fluid_tiles * ROWS, width), jnp.float32),
            pltpu.VMEM((owners * own_tiles * ROWS, width), jnp.float32),
        ],
        name="gather_terms",
    )(fluid_ids, solid_ids, flux, blocks)


def halves(value):
    high = value.astype(jnp.bfloat16)
    low = (value - high.astype(jnp.float32)).astype(jnp.bfloat16)
    return high, low


def stacked(value):
    both = jnp.concatenate(halves(value), axis=0)
    return jnp.concatenate([both, both], axis=1)


def folded(product):
    return product[:ROWS] + product[ROWS:]


def project_kernel(
    fluids, owners, offsets, parts, offset_rows, diag, couple, mapped_out, nodal_out,
    diag_f, couple_f, first, second, got_fluid, to_owner, got_owner, mapped,
    basis0, basis1, basis2, picks, spread, back, rim_out, rim_in, carry_out, carry_in, sums,
    load_sem, send1, recv1, send2, recv2, send3, recv3, send_rim, recv_rim,
    send_carry, recv_carry, send_sum, recv_sum,
):
    me_g = lax.axis_index("fluid")
    me_s = lax.axis_index("solid")
    fields = parts.shape[2]
    chunks = parts.shape[3]
    own_tiles = diag.shape[0]
    reach = own_tiles // 2
    own_rows = own_tiles * ROWS

    load_d = pltpu.make_async_copy(diag, diag_f, load_sem.at[0])
    load_c = pltpu.make_async_copy(couple, couple_f, load_sem.at[1])
    load_d.start()
    load_c.start()

    def fluid_peer(step):
        return lax.rem(me_g + step, fluids)

    def solid_peer(step):
        return lax.rem(me_s + step, owners)

    barrier = pltpu.get_barrier_semaphore()
    for step in range(1, fluids):
        pl.semaphore_signal(
            barrier, inc=1, device_id={"fluid": fluid_peer(step), "solid": me_s}, device_id_type=MESH
        )
    for step in range(1, owners):
        pl.semaphore_signal(
            barrier, inc=1, device_id={"fluid": me_g, "solid": solid_peer(step)}, device_id_type=MESH
        )
    pl.semaphore_wait(barrier, fluids - 1 + owners - 1)

    def remote(src, dst, send_sem, recv_sem, g, s):
        return pltpu.make_async_remote_copy(
            src_ref=src, dst_ref=dst, send_sem=send_sem, recv_sem=recv_sem,
            device_id={"fluid": g, "solid": s}, device_id_type=MESH,
        )

    def copy1(hop, step):
        owner = solid_peer(step)
        peer = fluid_peer(hop)
        return remote(
            parts.at[peer, owner], got_fluid.at[hop - 1, owner],
            send1.at[hop - 1, owner], recv1.at[hop - 1, owner], peer, me_s,
        )

    def copy2(step):
        owner = solid_peer(step)
        return remote(
            to_owner.at[step - 1], got_owner.at[step - 1],
            send2.at[step - 1], recv2.at[step - 1], me_g, owner,
        )

    def copy3(hop):
        return remote(
            mapped.at[me_g], mapped.at[me_g], send3.at[hop - 1], recv3.at[hop - 1], fluid_peer(hop), me_s
        )

    def copy_sum(step):
        return remote(
            sums.at[me_s], sums.at[me_s], send_sum.at[step - 1], recv_sum.at[step - 1],
            me_g, solid_peer(step),
        )

    for step in range(1, owners + 1):
        for hop in range(1, fluids):
            copy1(hop, step).start()

    basis0[...] = jnp.zeros_like(basis0)
    basis1[...] = jnp.zeros_like(basis1)
    basis2[...] = jnp.zeros_like(basis2)

    load_d.wait()
    load_c.wait()

    def prepare(tile, carry):
        diag_high, diag_low = halves(diag_f[tile])
        block = couple_f[tile]
        couple_high, couple_low = halves(block)
        turned_high, turned_low = halves(block.T)
        first[tile, :LANES, :LANES] = diag_high
        first[tile, LANES:, :LANES] = diag_low
        first[tile, :LANES, LANES:] = couple_high
        first[tile, LANES:, LANES:] = couple_low
        second[tile, :LANES, :] = turned_high
        second[tile, LANES:, :] = turned_low
        return carry

    lax.fori_loop(0, own_tiles, prepare, 0)

    for step in range(1, owners + 1):
        owner = solid_peer(step)
        for hop in range(1, fluids):
            copy1(hop, step).wait_recv()
        total = parts[me_g, owner]
        for hop in range(1, fluids):
            total = total + got_fluid[hop - 1, owner]
        if step < owners:
            to_owner[step - 1] = total
            copy2(step).start()
    for step in range(1, owners):
        copy2(step).wait_recv()
        total = total + got_owner[step - 1]
    mapped[me_g] = total
    for hop in range(1, fluids):
        copy3(hop).start()
    for hop in range(1, fluids):
        copy3(hop).wait_recv()
    for part in range(fluids):
        for field in range(fields):
            values = mapped[part, field]
            mapped_out[field, part * chunks : (part + 1) * chunks, :] = values
            basis0[pl.ds(part * chunks * ROWS + field, chunks, stride=ROWS), :] = values

    def rim_copy(turn):
        return remote(
            rim_out.at[turn], rim_in.at[turn], send_rim.at[turn], recv_rim.at[turn], me_g, me_s - 1
        )

    def carry_copy(turn):
        return remote(
            carry_out.at[turn], carry_in.at[turn], send_carry.at[turn], recv_carry.at[turn], me_g, me_s + 1
        )

    def send_rim_of(turn, vector):
        for field in range(fields):
            rim_out[turn, field] = vector[pl.ds(field, reach, stride=ROWS), :]

        @pl.when(me_s > 0)
        def _():
            rim_copy(turn).start()

    def take_rim(turn, vector):
        @pl.when(me_s < owners - 1)
        def _():
            rim_copy(turn).wait_recv()
            for field in range(fields):
                vector[pl.ds(own_rows + field, reach, stride=ROWS), :] = rim_in[turn, field]

        for tile in range(own_tiles + reach):
            picks[tile] = vector[tile * ROWS : (tile + 1) * ROWS, :]

    def rows_of(tile):
        return pl.ds(pl.multiple_of(tile * ROWS, ROWS), ROWS)

    def ahead_of(tile):
        picked = picks[tile + offsets[tile]]
        return folded(jnp.dot(stacked(picked), second[tile], preferred_element_type=jnp.float32))

    def apply_mass(turn, vector, image):
        send_rim_of(turn, vector)

        def own(tile, carry):
            product = folded(
                jnp.dot(stacked(vector[rows_of(tile), :]), first[tile], preferred_element_type=jnp.float32)
            )
            spread[rows_of(tile), :] = product[:, :LANES]
            back[rows_of(tile), :] = product[:, LANES:]
            return carry

        lax.fori_loop(0, own_tiles, own, 0, unroll=8)
        spread[own_rows:, :] = jnp.zeros((reach * ROWS, LANES), jnp.float32)

        def move(offset, carry):
            start = pl.multiple_of(offset * ROWS, ROWS)
            moved = jnp.where(offset_rows[...] == offset, back[...], 0.0)
            spread[pl.ds(start, own_rows), :] += moved
            return carry

        lax.fori_loop(1, reach + 1, move, 0)
        for field in range(fields):
            carry_out[turn, field] = spread[pl.ds(own_rows + field, reach, stride=ROWS), :]

        @pl.when(me_s < owners - 1)
        def _():
            carry_copy(turn).start()

        take_rim(turn, vector)

        def ahead(tile, carry):
            image[rows_of(tile), :] = spread[rows_of(tile), :] + ahead_of(tile)
            return carry

        lax.fori_loop(0, own_tiles, ahead, 0, unroll=8)

        @pl.when(me_s > 0)
        def _():
            carry_copy(turn).wait_recv()
            for field in range(fields):
                image[pl.ds(field, reach, stride=ROWS), :] += carry_in[turn, field]

    apply_mass(0, basis0, basis1)
    apply_mass(1, basis1, basis2)
    send_rim_of(2, basis2)

    def dots(tile, carry):
        zero, one, two = (b[rows_of(tile), :] for b in (basis0, basis1, basis2))
        product = folded(
            jnp.dot(stacked(two), first[tile, :, :LANES], preferred_element_type=jnp.float32)
        )
        pairs = ((zero, zero), (zero, one), (one, one), (one, two), (two, two), (two, product))
        return tuple(c + a * b for c, (a, b) in zip(carry, pairs))

    nothing = jnp.zeros((ROWS, LANES), jnp.float32)
    products = lax.fori_loop(0, own_tiles, dots, (nothing,) * 6, unroll=8)
    take_rim(2, basis2)

    def last(tile, carry):
        return carry + 2.0 * basis2[rows_of(tile), :] * ahead_of(tile)

    products = products[:5] + (lax.fori_loop(0, own_tiles, last, products[5], unroll=8),)
    lane = lax.broadcasted_iota(jnp.int32, (ROWS, LANES), 1)
    packed = nothing
    for place, product in enumerate(products):
        packed = jnp.where(lane == place, jnp.sum(product, axis=1, keepdims=True), packed)
    sums[me_s] = packed
    for step in range(1, owners):
        copy_sum(step).start()
    for step in range(1, owners):
        copy_sum(step).wait_recv()
    everyone = sums[0]
    for device in range(1, owners):
        everyone = everyone + sums[device]
    moments = [
        jnp.sum(jnp.where(lane == place, everyone, 0.0), axis=1, keepdims=True) for place in range(6)
    ]

    def form(coefficients, shift):
        total = None
        for i, left in enumerate(coefficients):
            for j, right in enumerate(coefficients):
                term = left * right * moments[i + j + shift]
                total = term if total is None else total + term
        return total

    alpha0 = moments[0] / moments[1]
    residual1 = (1.0, -alpha0)
    norm1 = form(residual1, 0)
    beta0 = norm1 / moments[0]
    direction1 = (1.0 + beta0, -alpha0)
    alpha1 = norm1 / form(direction1, 1)
    residual2 = (1.0, -alpha0 - alpha1 * direction1[0], -alpha1 * direction1[1])
    norm2 = form(residual2, 0)
    beta1 = norm2 / norm1
    direction2 = (
        residual2[0] + beta1 * direction1[0], residual2[1] + beta1 * direction1[1], residual2[2]
    )
    alpha2 = norm2 / form(direction2, 1)
    weights = (
        alpha0 + alpha1 * direction1[0] + alpha2 * direction2[0],
        alpha1 * direction1[1] + alpha2 * direction2[1],
        alpha2 * direction2[2],
    )
    for field in range(fields):
        result = None
        for weight, vector in zip(weights, (basis0, basis1, basis2)):
            term = weight[field : field + 1] * vector[pl.ds(field, own_tiles, stride=ROWS), :]
            result = term if result is None else result + term
        nodal_out[field] = result

    for step in range(1, owners + 1):
        for hop in range(1, fluids):
            copy1(hop, step).wait_send()
    for step in range(1, owners):
        copy2(step).wait_send()
        copy_sum(step).wait_send()
    for hop in range(1, fluids):
        copy3(hop).wait_send()

    @pl.when(me_s > 0)
    def _():
        for turn in range(3):
            rim_copy(turn).wait_send()

    @pl.when(me_s < owners - 1)
    def _():
        for turn in range(2):
            carry_copy(turn).wait_send()


def project(parts, diag, couple, offsets):
    fluids, owners, fields, chunks, width = parts.shape
    own_tiles = diag.shape[0]
    reach = own_tiles // 2
    offset_rows = jnp.broadcast_to(offsets[:, None, None], (own_tiles, ROWS, width))
    offset_rows = offset_rows.reshape(own_tiles * ROWS, width)
    f32, bf16 = jnp.float32, jnp.bfloat16
    dma = pltpu.SemaphoreType.DMA
    wide = (own_tiles + reach) * ROWS
    out = jax.ShapeDtypeStruct((fields, own_tiles, width), f32)
    vmem = pl.BlockSpec(memory_space=pltpu.VMEM)
    return pl.pallas_call(
        functools.partial(project_kernel, fluids, owners),
        out_shape=(out, out),
        in_specs=[
            pl.BlockSpec(memory_space=pltpu.SMEM), vmem, vmem,
            pl.BlockSpec(memory_space=pl.ANY), pl.BlockSpec(memory_space=pl.ANY),
        ],
        out_specs=(vmem, vmem),
        scratch_shapes=[
            pltpu.VMEM((own_tiles, width, width), f32),
            pltpu.VMEM((own_tiles, width, width), f32),
            pltpu.VMEM((own_tiles, 2 * width, 2 * width), bf16),
            pltpu.VMEM((own_tiles, 2 * width, width), bf16),
            pltpu.VMEM((fluids - 1, owners, fields, chunks, width), f32),
            pltpu.VMEM((owners - 1, fields, chunks, width), f32),
            pltpu.VMEM((owners - 1, fields, chunks, width), f32),
            pltpu.VMEM((fluids, fields, chunks, width), f32),
            pltpu.VMEM((wide, width), f32),
            pltpu.VMEM((wide, width), f32),
            pltpu.VMEM((wide, width), f32),
            pltpu.VMEM((own_tiles + reach, ROWS, width), f32),
            pltpu.VMEM((wide, width), f32),
            pltpu.VMEM((own_tiles * ROWS, width), f32),
            pltpu.VMEM((3, fields, reach, width), f32),
            pltpu.VMEM((3, fields, reach, width), f32),
            pltpu.VMEM((2, fields, reach, width), f32),
            pltpu.VMEM((2, fields, reach, width), f32),
            pltpu.VMEM((owners, ROWS, width), f32),
            dma((2,)),
            dma((fluids - 1, owners)), dma((fluids - 1, owners)),
            dma((owners - 1,)), dma((owners - 1,)),
            dma((fluids - 1,)), dma((fluids - 1,)),
            dma((3,)), dma((3,)),
            dma((2,)), dma((2,)),
            dma((owners - 1,)), dma((owners - 1,)),
        ],
        compiler_params=pltpu.CompilerParams(collective_id=0, has_side_effects=True),
        name="project",
    )(offsets, parts, offset_rows, diag, couple)


def local(
    fluid_flux, margin_blocks, block_fluid, block_solid, diag_blocks, couple_blocks, couple_offset
):
    fluids = lax.axis_size("fluid")
    owners = lax.axis_size("solid")
    parts = gather_terms(
        fluid_flux, margin_blocks, block_fluid, block_solid, fluids, owners, diag_blocks.shape[0]
    )
    return project(parts, diag_blocks, couple_blocks, couple_offset)


def solution(mesh):
    in_specs = (
        P(None, ("fluid", "solid"), None),
        P(("fluid", "solid"), None, None),
        P(("fluid", "solid")),
        P(("fluid", "solid")),
        P("solid", None, None),
        P("solid", None, None),
        P("solid"),
    )
    out_specs = (P(None, "solid", None), P(None, "solid", None))
    return jax.shard_map(local, mesh=mesh, in_specs=in_specs, out_specs=out_specs, check_vma=False)
```

```python
import functools

import jax
import jax.numpy as jnp
from jax import lax
from jax.experimental import pallas as pl
from jax.experimental.pallas import tpu as pltpu
from jax.sharding import PartitionSpec as P

MESH = pl.DeviceIdType.MESH
ROWS = 8
LANES = 128


def halves(value):
    high = value.astype(jnp.bfloat16)
    low = (value - high.astype(jnp.float32)).astype(jnp.bfloat16)
    return high, low


def thirds(value):
    high = value.astype(jnp.bfloat16)
    rest = value - high.astype(jnp.float32)
    middle = rest.astype(jnp.bfloat16)
    low = (rest - middle.astype(jnp.float32)).astype(jnp.bfloat16)
    return high, middle, low


def routed(onehot, value):
    return sum(jnp.dot(onehot, part, preferred_element_type=jnp.float32) for part in thirds(value))


def hits(condition):
    return jnp.where(condition, 1.0, 0.0).astype(jnp.bfloat16)


def stacked(value):
    both = jnp.concatenate(halves(value), axis=0)
    return jnp.concatenate([both, both], axis=1)


def folded(product):
    return product[:ROWS] + product[ROWS:]


def project_kernel(
    fluids, owners, offsets, fluid_ids, offset_row, solid_row, flux, blocks, diag, couple, outs,
    blocks_v, faces_flat, faces, terms, parts, diag_f, couple_f, first, second, got_fluid, to_owner, got_owner, mapped,
    basis0, basis1, basis2, picks, spread, back, rim_out, rim_in, carry_out, carry_in, sums,
    block_sem, load_sem, send1, recv1, send2, recv2, send3, recv3, send_rim, recv_rim,
    send_carry, recv_carry, send_sum, recv_sum,
):
    me_g = lax.axis_index("fluid")
    me_s = lax.axis_index("solid")
    fields = parts.shape[2]
    chunks = parts.shape[3]
    mapped_out, nodal_out = outs.at[0], outs.at[1]
    own_tiles = diag.shape[0]
    reach = own_tiles // 2
    own_rows = own_tiles * ROWS

    load_d = pltpu.make_async_copy(diag, diag_f, load_sem.at[0])
    load_c = pltpu.make_async_copy(couple, couple_f, load_sem.at[1])
    count, width = blocks.shape[0], blocks.shape[2]
    pieces = block_sem.shape[0]
    piece = count // pieces

    def load_block(index):
        span = pl.ds(index * piece, piece)
        return pltpu.make_async_copy(blocks.at[span], blocks_v.at[span], block_sem.at[index])

    for index in range(pieces):
        load_block(index).start()

    def fluid_peer(step):
        return lax.rem(me_g + step, fluids)

    def solid_peer(step):
        return lax.rem(me_s + step, owners)

    barrier = pltpu.get_barrier_semaphore()
    for step in range(1, fluids):
        pl.semaphore_signal(
            barrier, inc=1, device_id={"fluid": fluid_peer(step), "solid": me_s}, device_id_type=MESH
        )
    for step in range(1, owners):
        pl.semaphore_signal(
            barrier, inc=1, device_id={"fluid": me_g, "solid": solid_peer(step)}, device_id_type=MESH
        )

    faces_flat[...] = jnp.zeros_like(faces_flat)
    for field in range(fields):
        faces_flat[pl.ds(field, flux.shape[1], stride=ROWS), :] = flux[field].astype(jnp.float32)
    for tile in range(flux.shape[1]):
        faces[tile] = faces_flat[tile * ROWS : (tile + 1) * ROWS, :]
    basis0[...] = jnp.zeros_like(basis0)
    basis1[...] = jnp.zeros_like(basis1)
    basis2[...] = jnp.zeros_like(basis2)

    for index in range(pieces):
        load_block(index).wait()
        if index == pieces // 2:
            load_d.start()
            load_c.start()

        def one_term(block, carry):
            chosen = faces[fluid_ids[block]].astype(jnp.bfloat16)
            term = jnp.dot(chosen, blocks_v[block], preferred_element_type=jnp.float32)
            terms[pl.ds(pl.multiple_of(block * ROWS, ROWS), ROWS), :] = term
            return carry

        lax.fori_loop(index * piece, (index + 1) * piece, one_term, 0, unroll=16)

    table = jnp.concatenate(
        [terms[pl.ds(field, count, stride=ROWS), :] for field in range(fields)], axis=1
    )
    span = own_tiles * max(1, min(owners, 256 // own_tiles))
    for base in range(0, owners * own_tiles, span):
        tiles = lax.broadcasted_iota(jnp.int32, (span, count), 0) + base
        summed = routed(hits(tiles == solid_row[...]), table)
        for start in range(0, span, chunks):
            owner, part = (base + start) // own_tiles, start % own_tiles // chunks
            for field in range(fields):
                parts[part, owner, field] = summed[
                    start : start + chunks, field * width : (field + 1) * width
                ]
    pl.semaphore_wait(barrier, fluids - 1 + owners - 1)

    def remote(src, dst, send_sem, recv_sem, g, s):
        return pltpu.make_async_remote_copy(
            src_ref=src, dst_ref=dst, send_sem=send_sem, recv_sem=recv_sem,
            device_id={"fluid": g, "solid": s}, device_id_type=MESH,
        )

    def copy1(hop, step):
        owner = solid_peer(step)
        peer = fluid_peer(hop)
        return remote(
            parts.at[peer, owner], got_fluid.at[hop - 1, owner],
            send1.at[hop - 1, owner], recv1.at[hop - 1, owner], peer, me_s,
        )

    def copy2(step):
        owner = solid_peer(step)
        return remote(
            to_owner.at[step - 1], got_owner.at[step - 1],
            send2.at[step - 1], recv2.at[step - 1], me_g, owner,
        )

    def copy3(hop):
        return remote(
            mapped.at[me_g], mapped.at[me_g], send3.at[hop - 1], recv3.at[hop - 1], fluid_peer(hop), me_s
        )

    def copy_sum(step):
        return remote(
            sums.at[me_s], sums.at[me_s], send_sum.at[step - 1], recv_sum.at[step - 1],
            me_g, solid_peer(step),
        )

    for step in range(1, owners + 1):
        for hop in range(1, fluids):
            copy1(hop, step).start()

    load_d.wait()
    load_c.wait()

    def prepare(tile, carry):
        diag_high, diag_low = halves(diag_f[tile])
        block = couple_f[tile]
        couple_high, couple_low = halves(block)
        turned_high, turned_low = halves(block.T)
        first[tile, :LANES, :LANES] = diag_high
        first[tile, LANES:, :LANES] = diag_low
        first[tile, :LANES, LANES:] = couple_high
        first[tile, LANES:, LANES:] = couple_low
        second[tile, :LANES, :] = turned_high
        second[tile, LANES:, :] = turned_low
        return carry

    lax.fori_loop(0, own_tiles, prepare, 0, unroll=4)

    for step in range(1, owners + 1):
        owner = solid_peer(step)
        for hop in range(1, fluids):
            copy1(hop, step).wait_recv()
        total = parts[me_g, owner]
        for hop in range(1, fluids):
            total = total + got_fluid[hop - 1, owner]
        if step < owners:
            to_owner[step - 1] = total
            copy2(step).start()
    for step in range(1, owners):
        copy2(step).wait_recv()
        total = total + got_owner[step - 1]
    mapped[me_g] = total
    for hop in range(1, fluids):
        copy3(hop).start()
    for hop in range(1, fluids):
        copy3(hop).wait_recv()
    for part in range(fluids):
        for field in range(fields):
            values = mapped[part, field]
            mapped_out[field, part * chunks : (part + 1) * chunks, :] = values
            basis0[pl.ds(part * chunks * ROWS + field, chunks, stride=ROWS), :] = values

    def rim_copy(turn):
        return remote(
            rim_out.at[turn], rim_in.at[turn], send_rim.at[turn], recv_rim.at[turn], me_g, me_s - 1
        )

    def carry_copy(turn):
        return remote(
            carry_out.at[turn], carry_in.at[turn], send_carry.at[turn], recv_carry.at[turn], me_g, me_s + 1
        )

    def send_rim_of(turn, vector):
        for field in range(fields):
            rim_out[turn, field] = vector[pl.ds(field, reach, stride=ROWS), :]

        @pl.when(me_s > 0)
        def _():
            rim_copy(turn).start()

    def take_rim(turn, vector):
        @pl.when(me_s < owners - 1)
        def _():
            rim_copy(turn).wait_recv()
            for field in range(fields):
                vector[pl.ds(own_rows + field, reach, stride=ROWS), :] = rim_in[turn, field]

        for tile in range(own_tiles + reach):
            picks[tile] = vector[tile * ROWS : (tile + 1) * ROWS, :]

    def rows_of(tile):
        return pl.ds(pl.multiple_of(tile * ROWS, ROWS), ROWS)

    def ahead_of(tile):
        picked = picks[tile + offsets[tile]]
        return folded(jnp.dot(stacked(picked), second[tile], preferred_element_type=jnp.float32))

    def apply_mass(turn, vector, image):
        send_rim_of(turn, vector)

        def own(tile, carry):
            product = folded(
                jnp.dot(stacked(vector[rows_of(tile), :]), first[tile], preferred_element_type=jnp.float32)
            )
            spread[rows_of(tile), :] = product[:, :LANES]
            back[rows_of(tile), :] = product[:, LANES:]
            return carry

        lax.fori_loop(0, own_tiles, own, 0, unroll=16)
        table = jnp.concatenate(
            [back[pl.ds(field, own_tiles, stride=ROWS), :] for field in range(fields)], axis=1
        )
        targets = lax.broadcasted_iota(jnp.int32, (own_tiles + reach, own_tiles), 0)
        sources = lax.broadcasted_iota(jnp.int32, (own_tiles + reach, own_tiles), 1)
        moved = routed(hits(sources + offset_row[...] == targets), table)
        for field in range(fields):
            lanes = slice(field * LANES, (field + 1) * LANES)
            carry_out[turn, field] = moved[own_tiles:, lanes]
            spread[pl.ds(field, own_tiles, stride=ROWS), :] += moved[:own_tiles, lanes]

        @pl.when(me_s < owners - 1)
        def _():
            carry_copy(turn).start()

        take_rim(turn, vector)

        def ahead(tile, carry):
            image[rows_of(tile), :] = spread[rows_of(tile), :] + ahead_of(tile)
            return carry

        lax.fori_loop(0, own_tiles, ahead, 0, unroll=16)

        @pl.when(me_s > 0)
        def _():
            carry_copy(turn).wait_recv()
            for field in range(fields):
                image[pl.ds(field, reach, stride=ROWS), :] += carry_in[turn, field]

    apply_mass(0, basis0, basis1)
    apply_mass(1, basis1, basis2)
    send_rim_of(2, basis2)

    def dots(tile, carry):
        zero, one, two = (b[rows_of(tile), :] for b in (basis0, basis1, basis2))
        product = folded(
            jnp.dot(stacked(two), first[tile, :, :LANES], preferred_element_type=jnp.float32)
        )
        pairs = ((zero, zero), (zero, one), (one, one), (one, two), (two, two), (two, product))
        return tuple(c + a * b for c, (a, b) in zip(carry, pairs))

    nothing = jnp.zeros((ROWS, LANES), jnp.float32)
    products = lax.fori_loop(0, own_tiles, dots, (nothing,) * 6, unroll=16)
    take_rim(2, basis2)

    def last(tile, carry):
        return carry + 2.0 * basis2[rows_of(tile), :] * ahead_of(tile)

    products = products[:5] + (lax.fori_loop(0, own_tiles, last, products[5], unroll=16),)
    lane = lax.broadcasted_iota(jnp.int32, (ROWS, LANES), 1)
    packed = nothing
    for place, product in enumerate(products):
        packed = jnp.where(lane == place, jnp.sum(product, axis=1, keepdims=True), packed)
    sums[me_s] = packed
    for step in range(1, owners):
        copy_sum(step).start()
    for step in range(1, owners):
        copy_sum(step).wait_recv()
    everyone = sums[0]
    for device in range(1, owners):
        everyone = everyone + sums[device]
    moments = [
        jnp.sum(jnp.where(lane == place, everyone, 0.0), axis=1, keepdims=True) for place in range(6)
    ]

    def form(coefficients, shift):
        total = None
        for i, left in enumerate(coefficients):
            for j, right in enumerate(coefficients):
                term = left * right * moments[i + j + shift]
                total = term if total is None else total + term
        return total

    alpha0 = moments[0] / moments[1]
    residual1 = (1.0, -alpha0)
    norm1 = form(residual1, 0)
    beta0 = norm1 / moments[0]
    direction1 = (1.0 + beta0, -alpha0)
    alpha1 = norm1 / form(direction1, 1)
    residual2 = (1.0, -alpha0 - alpha1 * direction1[0], -alpha1 * direction1[1])
    norm2 = form(residual2, 0)
    beta1 = norm2 / norm1
    direction2 = (
        residual2[0] + beta1 * direction1[0], residual2[1] + beta1 * direction1[1], residual2[2]
    )
    alpha2 = norm2 / form(direction2, 1)
    weights = (
        alpha0 + alpha1 * direction1[0] + alpha2 * direction2[0],
        alpha1 * direction1[1] + alpha2 * direction2[1],
        alpha2 * direction2[2],
    )
    for field in range(fields):
        result = None
        for weight, vector in zip(weights, (basis0, basis1, basis2)):
            term = weight[field : field + 1] * vector[pl.ds(field, own_tiles, stride=ROWS), :]
            result = term if result is None else result + term
        nodal_out[field] = result

    for step in range(1, owners + 1):
        for hop in range(1, fluids):
            copy1(hop, step).wait_send()
    for step in range(1, owners):
        copy2(step).wait_send()
        copy_sum(step).wait_send()
    for hop in range(1, fluids):
        copy3(hop).wait_send()

    @pl.when(me_s > 0)
    def _():
        for turn in range(3):
            rim_copy(turn).wait_send()

    @pl.when(me_s < owners - 1)
    def _():
        for turn in range(2):
            carry_copy(turn).wait_send()


def finish_kernel(both, mapped_out, nodal_out):
    mapped_out[...] = both[0]
    nodal_out[...] = both[1]


def local(
    fluid_flux, margin_blocks, block_fluid, block_solid, diag_blocks, couple_blocks, couple_offset
):
    fluids = lax.axis_size("fluid")
    owners = lax.axis_size("solid")
    fields, fluid_tiles, width = fluid_flux.shape
    count = margin_blocks.shape[0]
    own_tiles = diag_blocks.shape[0]
    chunks = own_tiles // fluids
    reach = own_tiles // 2
    pieces = count // 32 if count % 32 == 0 else 1
    f32, bf16 = jnp.float32, jnp.bfloat16
    dma = pltpu.SemaphoreType.DMA
    wide = (own_tiles + reach) * ROWS
    vmem = pl.BlockSpec(memory_space=pltpu.VMEM)
    smem = pl.BlockSpec(memory_space=pltpu.SMEM)
    far = pl.BlockSpec(memory_space=pltpu.HBM)
    both = pl.pallas_call(
        functools.partial(project_kernel, fluids, owners),
        out_shape=jax.ShapeDtypeStruct((2, fields, own_tiles, width), f32),
        in_specs=[smem, smem, vmem, vmem, vmem, far, far, far],
        out_specs=vmem,
        scratch_shapes=[
            pltpu.VMEM((count, width, width), bf16),
            pltpu.VMEM((fluid_tiles * ROWS, width), f32),
            pltpu.VMEM((fluid_tiles, ROWS, width), f32),
            pltpu.VMEM((count * ROWS, width), f32),
            pltpu.VMEM((fluids, owners, fields, chunks, width), f32),
            pltpu.VMEM((own_tiles, width, width), f32),
            pltpu.VMEM((own_tiles, width, width), f32),
            pltpu.VMEM((own_tiles, 2 * width, 2 * width), bf16),
            pltpu.VMEM((own_tiles, 2 * width, width), bf16),
            pltpu.VMEM((fluids - 1, owners, fields, chunks, width), f32),
            pltpu.VMEM((owners - 1, fields, chunks, width), f32),
            pltpu.VMEM((owners - 1, fields, chunks, width), f32),
            pltpu.VMEM((fluids, fields, chunks, width), f32),
            pltpu.VMEM((wide, width), f32),
            pltpu.VMEM((wide, width), f32),
            pltpu.VMEM((wide, width), f32),
            pltpu.VMEM((own_tiles + reach, ROWS, width), f32),
            pltpu.VMEM((own_tiles * ROWS, width), f32),
            pltpu.VMEM((own_tiles * ROWS, width), f32),
            pltpu.VMEM((3, fields, reach, width), f32),
            pltpu.VMEM((3, fields, reach, width), f32),
            pltpu.VMEM((2, fields, reach, width), f32),
            pltpu.VMEM((2, fields, reach, width), f32),
            pltpu.VMEM((owners, ROWS, width), f32),
            dma((pieces,)),
            dma((2,)),
            dma((fluids - 1, owners)), dma((fluids - 1, owners)),
            dma((owners - 1,)), dma((owners - 1,)),
            dma((fluids - 1,)), dma((fluids - 1,)),
            dma((3,)), dma((3,)),
            dma((2,)), dma((2,)),
            dma((owners - 1,)), dma((owners - 1,)),
        ],
        compiler_params=pltpu.CompilerParams(
            collective_id=0, has_side_effects=True, vmem_limit_bytes=62400 * 1024
        ),
        name="project",
    )(
        couple_offset, block_fluid, couple_offset[None, :], block_solid[None, :],
        fluid_flux, margin_blocks, diag_blocks, couple_blocks,
    )
    out = jax.ShapeDtypeStruct((fields, own_tiles, width), f32)
    return pl.pallas_call(
        finish_kernel, out_shape=(out, out), in_specs=[vmem], out_specs=(vmem, vmem), name="finish",
        compiler_params=pltpu.CompilerParams(vmem_limit_bytes=8 * 1024 * 1024),
    )(both)


def solution(mesh):
    in_specs = (
        P(None, ("fluid", "solid"), None),
        P(("fluid", "solid"), None, None),
        P(("fluid", "solid")),
        P(("fluid", "solid")),
        P("solid", None, None),
        P("solid", None, None),
        P("solid"),
    )
    out_specs = (P(None, "solid", None), P(None, "solid", None))
    return jax.shard_map(local, mesh=mesh, in_specs=in_specs, out_specs=out_specs, check_vma=False)
```

```python
import functools

import jax
import jax.numpy as jnp
from jax import lax
from jax.experimental import pallas as pl
from jax.experimental.pallas import tpu as pltpu
from jax.sharding import PartitionSpec as P

MESH = pl.DeviceIdType.MESH
ROWS = 8
LANES = 128


def halves(value):
    high = value.astype(jnp.bfloat16)
    low = (value - high.astype(jnp.float32)).astype(jnp.bfloat16)
    return high, low


def thirds(value):
    high = value.astype(jnp.bfloat16)
    rest = value - high.astype(jnp.float32)
    middle = rest.astype(jnp.bfloat16)
    low = (rest - middle.astype(jnp.float32)).astype(jnp.bfloat16)
    return high, middle, low


def routed(onehot, value):
    return sum(jnp.dot(onehot, part, preferred_element_type=jnp.float32) for part in thirds(value))


def hits(condition):
    return jnp.where(condition, 1.0, 0.0).astype(jnp.bfloat16)


def stacked(value):
    both = jnp.concatenate(halves(value), axis=0)
    return jnp.concatenate([both, both], axis=1)


def folded(product):
    return product[:ROWS] + product[ROWS:]


def project_kernel(
    fluids, owners, offsets, fluid_ids, offset_row, solid_row, flux, blocks, diag, couple, outs,
    blocks_v, faces_flat, faces, terms, parts, diag_f, couple_f, first, second, got_fluid, to_owner, got_owner, mapped,
    basis0, basis1, basis2, picks, spread, back, rim_out, rim_in, carry_out, carry_in, sums,
    block_sem, load_sem, send1, recv1, send2, recv2, send3, recv3, send_rim, recv_rim,
    send_carry, recv_carry, send_sum, recv_sum,
):
    me_g = lax.axis_index("fluid")
    me_s = lax.axis_index("solid")
    fields = parts.shape[2]
    chunks = parts.shape[3]
    mapped_out, nodal_out = outs.at[0], outs.at[1]
    own_tiles = diag.shape[0]
    reach = own_tiles // 2
    own_rows = own_tiles * ROWS

    load_d = pltpu.make_async_copy(diag, diag_f, load_sem.at[0])
    load_c = pltpu.make_async_copy(couple, couple_f, load_sem.at[1])
    count, width = blocks.shape[0], blocks.shape[2]
    pieces = block_sem.shape[0]
    piece = count // pieces

    def load_block(index):
        span = pl.ds(index * piece, piece)
        return pltpu.make_async_copy(blocks.at[span], blocks_v.at[span], block_sem.at[index])

    for index in range(pieces):
        load_block(index).start()

    def fluid_peer(step):
        return lax.rem(me_g + step, fluids)

    def solid_peer(step):
        return lax.rem(me_s + step, owners)

    barrier = pltpu.get_barrier_semaphore()
    for step in range(1, fluids):
        pl.semaphore_signal(
            barrier, inc=1, device_id={"fluid": fluid_peer(step), "solid": me_s}, device_id_type=MESH
        )
    for step in range(1, owners):
        pl.semaphore_signal(
            barrier, inc=1, device_id={"fluid": me_g, "solid": solid_peer(step)}, device_id_type=MESH
        )

    faces_flat[...] = jnp.zeros_like(faces_flat)
    for field in range(fields):
        faces_flat[pl.ds(field, flux.shape[1], stride=ROWS), :] = flux[field].astype(jnp.float32)
    for tile in range(flux.shape[1]):
        faces[tile] = faces_flat[tile * ROWS : (tile + 1) * ROWS, :]
    basis0[...] = jnp.zeros_like(basis0)
    basis1[...] = jnp.zeros_like(basis1)
    basis2[...] = jnp.zeros_like(basis2)

    for index in range(pieces):
        load_block(index).wait()
        if index == pieces // 2:
            load_d.start()
            load_c.start()

        def one_term(block, carry):
            chosen = faces[fluid_ids[block]].astype(jnp.bfloat16)
            term = jnp.dot(chosen, blocks_v[block], preferred_element_type=jnp.float32)
            terms[pl.ds(pl.multiple_of(block * ROWS, ROWS), ROWS), :] = term
            return carry

        lax.fori_loop(index * piece, (index + 1) * piece, one_term, 0, unroll=32)

    table = jnp.concatenate(
        [terms[pl.ds(field, count, stride=ROWS), :] for field in range(fields)], axis=1
    )
    span = own_tiles * max(1, min(owners, 256 // own_tiles))
    for base in range(0, owners * own_tiles, span):
        tiles = lax.broadcasted_iota(jnp.int32, (span, count), 0) + base
        summed = routed(hits(tiles == solid_row[...]), table)
        for start in range(0, span, chunks):
            owner, part = (base + start) // own_tiles, start % own_tiles // chunks
            for field in range(fields):
                parts[part, owner, field] = summed[
                    start : start + chunks, field * width : (field + 1) * width
                ]
    pl.semaphore_wait(barrier, fluids - 1 + owners - 1)

    def remote(src, dst, send_sem, recv_sem, g, s):
        return pltpu.make_async_remote_copy(
            src_ref=src, dst_ref=dst, send_sem=send_sem, recv_sem=recv_sem,
            device_id={"fluid": g, "solid": s}, device_id_type=MESH,
        )

    def copy1(hop, step):
        owner = solid_peer(step)
        peer = fluid_peer(hop)
        return remote(
            parts.at[peer, owner], got_fluid.at[hop - 1, owner],
            send1.at[hop - 1, owner], recv1.at[hop - 1, owner], peer, me_s,
        )

    def copy2(step):
        owner = solid_peer(step)
        return remote(
            to_owner.at[step - 1], got_owner.at[step - 1],
            send2.at[step - 1], recv2.at[step - 1], me_g, owner,
        )

    def copy3(hop):
        return remote(
            mapped.at[me_g], mapped.at[me_g], send3.at[hop - 1], recv3.at[hop - 1], fluid_peer(hop), me_s
        )

    def copy_sum(step):
        return remote(
            sums.at[me_s], sums.at[me_s], send_sum.at[step - 1], recv_sum.at[step - 1],
            me_g, solid_peer(step),
        )

    for step in range(1, owners + 1):
        for hop in range(1, fluids):
            copy1(hop, step).start()

    load_d.wait()
    load_c.wait()

    def prepare(tile, carry):
        diag_high, diag_low = halves(diag_f[tile])
        block = couple_f[tile]
        couple_high, couple_low = halves(block)
        turned_high, turned_low = halves(block.T)
        first[tile, :LANES, :LANES] = diag_high
        first[tile, LANES:, :LANES] = diag_low
        first[tile, :LANES, LANES:] = couple_high
        first[tile, LANES:, LANES:] = couple_low
        second[tile, :LANES, :] = turned_high
        second[tile, LANES:, :] = turned_low
        return carry

    lax.fori_loop(0, own_tiles, prepare, 0, unroll=8)

    for step in range(1, owners + 1):
        owner = solid_peer(step)
        for hop in range(1, fluids):
            copy1(hop, step).wait_recv()
        total = parts[me_g, owner]
        for hop in range(1, fluids):
            total = total + got_fluid[hop - 1, owner]
        if step < owners:
            to_owner[step - 1] = total
            copy2(step).start()
    for step in range(1, owners):
        copy2(step).wait_recv()
        total = total + got_owner[step - 1]
    mapped[me_g] = total
    for hop in range(1, fluids):
        copy3(hop).start()
    for hop in range(1, fluids):
        copy3(hop).wait_recv()
    for part in range(fluids):
        for field in range(fields):
            values = mapped[part, field]
            mapped_out[field, part * chunks : (part + 1) * chunks, :] = values
            basis0[pl.ds(part * chunks * ROWS + field, chunks, stride=ROWS), :] = values

    def rim_copy(turn):
        return remote(
            rim_out.at[turn], rim_in.at[turn], send_rim.at[turn], recv_rim.at[turn], me_g, me_s - 1
        )

    def carry_copy(turn):
        return remote(
            carry_out.at[turn], carry_in.at[turn], send_carry.at[turn], recv_carry.at[turn], me_g, me_s + 1
        )

    def send_rim_of(turn, vector):
        for field in range(fields):
            rim_out[turn, field] = vector[pl.ds(field, reach, stride=ROWS), :]

        @pl.when(me_s > 0)
        def _():
            rim_copy(turn).start()

    def take_rim(turn, vector):
        @pl.when(me_s < owners - 1)
        def _():
            rim_copy(turn).wait_recv()
            for field in range(fields):
                vector[pl.ds(own_rows + field, reach, stride=ROWS), :] = rim_in[turn, field]

        for tile in range(own_tiles + reach):
            picks[tile] = vector[tile * ROWS : (tile + 1) * ROWS, :]

    def rows_of(tile):
        return pl.ds(pl.multiple_of(tile * ROWS, ROWS), ROWS)

    def ahead_of(tile):
        picked = picks[tile + offsets[tile]]
        return folded(jnp.dot(stacked(picked), second[tile], preferred_element_type=jnp.float32))

    def apply_mass(turn, vector, image):
        send_rim_of(turn, vector)

        def own(tile, carry):
            product = folded(
                jnp.dot(stacked(vector[rows_of(tile), :]), first[tile], preferred_element_type=jnp.float32)
            )
            spread[rows_of(tile), :] = product[:, :LANES]
            back[rows_of(tile), :] = product[:, LANES:]
            return carry

        lax.fori_loop(0, own_tiles, own, 0, unroll=32)
        table = jnp.concatenate(
            [back[pl.ds(field, own_tiles, stride=ROWS), :] for field in range(fields)], axis=1
        )
        targets = lax.broadcasted_iota(jnp.int32, (own_tiles + reach, own_tiles), 0)
        sources = lax.broadcasted_iota(jnp.int32, (own_tiles + reach, own_tiles), 1)
        moved = routed(hits(sources + offset_row[...] == targets), table)
        for field in range(fields):
            lanes = slice(field * LANES, (field + 1) * LANES)
            carry_out[turn, field] = moved[own_tiles:, lanes]
            spread[pl.ds(field, own_tiles, stride=ROWS), :] += moved[:own_tiles, lanes]

        @pl.when(me_s < owners - 1)
        def _():
            carry_copy(turn).start()

        take_rim(turn, vector)

        def ahead(tile, carry):
            image[rows_of(tile), :] = spread[rows_of(tile), :] + ahead_of(tile)
            return carry

        lax.fori_loop(0, own_tiles, ahead, 0, unroll=32)

        @pl.when(me_s > 0)
        def _():
            carry_copy(turn).wait_recv()
            for field in range(fields):
                image[pl.ds(field, reach, stride=ROWS), :] += carry_in[turn, field]

    apply_mass(0, basis0, basis1)
    apply_mass(1, basis1, basis2)
    send_rim_of(2, basis2)

    def dots(tile, carry):
        zero, one, two = (b[rows_of(tile), :] for b in (basis0, basis1, basis2))
        product = folded(
            jnp.dot(stacked(two), first[tile, :, :LANES], preferred_element_type=jnp.float32)
        )
        pairs = ((zero, zero), (zero, one), (one, one), (one, two), (two, two), (two, product))
        return tuple(c + a * b for c, (a, b) in zip(carry, pairs))

    nothing = jnp.zeros((ROWS, LANES), jnp.float32)
    products = lax.fori_loop(0, own_tiles, dots, (nothing,) * 6, unroll=32)
    take_rim(2, basis2)

    def last(tile, carry):
        return carry + 2.0 * basis2[rows_of(tile), :] * ahead_of(tile)

    products = products[:5] + (lax.fori_loop(0, own_tiles, last, products[5], unroll=32),)
    lane = lax.broadcasted_iota(jnp.int32, (ROWS, LANES), 1)
    packed = nothing
    for place, product in enumerate(products):
        packed = jnp.where(lane == place, jnp.sum(product, axis=1, keepdims=True), packed)
    sums[me_s] = packed
    for step in range(1, owners):
        copy_sum(step).start()
    for step in range(1, owners):
        copy_sum(step).wait_recv()
    everyone = sums[0]
    for device in range(1, owners):
        everyone = everyone + sums[device]
    moments = [
        jnp.sum(jnp.where(lane == place, everyone, 0.0), axis=1, keepdims=True) for place in range(6)
    ]

    def form(coefficients, shift):
        total = None
        for i, left in enumerate(coefficients):
            for j, right in enumerate(coefficients):
                term = left * right * moments[i + j + shift]
                total = term if total is None else total + term
        return total

    alpha0 = moments[0] / moments[1]
    residual1 = (1.0, -alpha0)
    norm1 = form(residual1, 0)
    beta0 = norm1 / moments[0]
    direction1 = (1.0 + beta0, -alpha0)
    alpha1 = norm1 / form(direction1, 1)
    residual2 = (1.0, -alpha0 - alpha1 * direction1[0], -alpha1 * direction1[1])
    norm2 = form(residual2, 0)
    beta1 = norm2 / norm1
    direction2 = (
        residual2[0] + beta1 * direction1[0], residual2[1] + beta1 * direction1[1], residual2[2]
    )
    alpha2 = norm2 / form(direction2, 1)
    weights = (
        alpha0 + alpha1 * direction1[0] + alpha2 * direction2[0],
        alpha1 * direction1[1] + alpha2 * direction2[1],
        alpha2 * direction2[2],
    )
    for field in range(fields):
        result = None
        for weight, vector in zip(weights, (basis0, basis1, basis2)):
            term = weight[field : field + 1] * vector[pl.ds(field, own_tiles, stride=ROWS), :]
            result = term if result is None else result + term
        nodal_out[field] = result

    for step in range(1, owners + 1):
        for hop in range(1, fluids):
            copy1(hop, step).wait_send()
    for step in range(1, owners):
        copy2(step).wait_send()
        copy_sum(step).wait_send()
    for hop in range(1, fluids):
        copy3(hop).wait_send()

    @pl.when(me_s > 0)
    def _():
        for turn in range(3):
            rim_copy(turn).wait_send()

    @pl.when(me_s < owners - 1)
    def _():
        for turn in range(2):
            carry_copy(turn).wait_send()


def finish_kernel(both, mapped_out, nodal_out):
    mapped_out[...] = both[0]
    nodal_out[...] = both[1]


def local(
    fluid_flux, margin_blocks, block_fluid, block_solid, diag_blocks, couple_blocks, couple_offset
):
    fluids = lax.axis_size("fluid")
    owners = lax.axis_size("solid")
    fields, fluid_tiles, width = fluid_flux.shape
    count = margin_blocks.shape[0]
    own_tiles = diag_blocks.shape[0]
    chunks = own_tiles // fluids
    reach = own_tiles // 2
    pieces = count // 32 if count % 32 == 0 else 1
    f32, bf16 = jnp.float32, jnp.bfloat16
    dma = pltpu.SemaphoreType.DMA
    wide = (own_tiles + reach) * ROWS
    vmem = pl.BlockSpec(memory_space=pltpu.VMEM)
    smem = pl.BlockSpec(memory_space=pltpu.SMEM)
    far = pl.BlockSpec(memory_space=pltpu.HBM)
    both = pl.pallas_call(
        functools.partial(project_kernel, fluids, owners),
        out_shape=jax.ShapeDtypeStruct((2, fields, own_tiles, width), f32),
        in_specs=[smem, smem, vmem, vmem, vmem, far, far, far],
        out_specs=vmem,
        scratch_shapes=[
            pltpu.VMEM((count, width, width), bf16),
            pltpu.VMEM((fluid_tiles * ROWS, width), f32),
            pltpu.VMEM((fluid_tiles, ROWS, width), f32),
            pltpu.VMEM((count * ROWS, width), f32),
            pltpu.VMEM((fluids, owners, fields, chunks, width), f32),
            pltpu.VMEM((own_tiles, width, width), f32),
            pltpu.VMEM((own_tiles, width, width), f32),
            pltpu.VMEM((own_tiles, 2 * width, 2 * width), bf16),
            pltpu.VMEM((own_tiles, 2 * width, width), bf16),
            pltpu.VMEM((fluids - 1, owners, fields, chunks, width), f32),
            pltpu.VMEM((owners - 1, fields, chunks, width), f32),
            pltpu.VMEM((owners - 1, fields, chunks, width), f32),
            pltpu.VMEM((fluids, fields, chunks, width), f32),
            pltpu.VMEM((wide, width), f32),
            pltpu.VMEM((wide, width), f32),
            pltpu.VMEM((wide, width), f32),
            pltpu.VMEM((own_tiles + reach, ROWS, width), f32),
            pltpu.VMEM((own_tiles * ROWS, width), f32),
            pltpu.VMEM((own_tiles * ROWS, width), f32),
            pltpu.VMEM((3, fields, reach, width), f32),
            pltpu.VMEM((3, fields, reach, width), f32),
            pltpu.VMEM((2, fields, reach, width), f32),
            pltpu.VMEM((2, fields, reach, width), f32),
            pltpu.VMEM((owners, ROWS, width), f32),
            dma((pieces,)),
            dma((2,)),
            dma((fluids - 1, owners)), dma((fluids - 1, owners)),
            dma((owners - 1,)), dma((owners - 1,)),
            dma((fluids - 1,)), dma((fluids - 1,)),
            dma((3,)), dma((3,)),
            dma((2,)), dma((2,)),
            dma((owners - 1,)), dma((owners - 1,)),
        ],
        compiler_params=pltpu.CompilerParams(
            collective_id=0, has_side_effects=True, vmem_limit_bytes=62400 * 1024
        ),
        name="project",
    )(
        couple_offset, block_fluid, couple_offset[None, :], block_solid[None, :],
        fluid_flux, margin_blocks, diag_blocks, couple_blocks,
    )
    out = jax.ShapeDtypeStruct((fields, own_tiles, width), f32)
    return pl.pallas_call(
        finish_kernel, out_shape=(out, out), in_specs=[vmem], out_specs=(vmem, vmem), name="finish",
        compiler_params=pltpu.CompilerParams(vmem_limit_bytes=8 * 1024 * 1024),
    )(both)


def solution(mesh):
    in_specs = (
        P(None, ("fluid", "solid"), None),
        P(("fluid", "solid"), None, None),
        P(("fluid", "solid")),
        P(("fluid", "solid")),
        P("solid", None, None),
        P("solid", None, None),
        P("solid"),
    )
    out_specs = (P(None, "solid", None), P(None, "solid", None))
    return jax.shard_map(local, mesh=mesh, in_specs=in_specs, out_specs=out_specs, check_vma=False)
```
